256 devices in a mesh: group: 4 (over z_hi, core), fsdp: 64 (over x, z_lo, y).
Axes of the slice: x: 4, y: 4, z: 8 (z_hi: 2, z_lo: 4; z = z_hi * 4 + z_lo), core: 2. Of those that a mesh axis runs over, the one named last changes fastest.
Arguments:
- tokens: bfloat16 [4, 40960, 8192], P('group', 'fsdp'), may hold values from -16 to 16
- keys_grad: bfloat16 [4, 40960, 512], P('group', 'fsdp'), may hold values from -6 to 6
- norm_gain: float32 [8192], replicated, may hold values from 0.5 to 1.5
- weight: bfloat16 [8192, 512], P('fsdp'), may hold values from -6 to 6
- momentum: float32 [8192, 512], P('fsdp', 'group'), may hold values from -6 to 6
Outputs:
- new_weight: bfloat16 [8192, 512], P('fsdp')
- new_momentum: float32 [8192, 512], P('fsdp', 'group')
The draws below stay inside these ranges and needn't reach their ends.
All inputs are finite; a program needn't handle non-finite values. Where the reference program divides by a largest or mean magnitude, that divisor is 1e-20 or more.
Results may differ from the reference program's by a relative error of at most 0.0066.
Values may be sent and summed in bfloat16 or wider, within the bound.
No kernel may reach another device: no remote copies, remote signals or barrier semaphores. Data moves between devices by JAX's collectives and lax.ppermute only.
A program may use at most 128 MiB of HBM per device.

```python
import math
import jax
import jax.numpy as jnp
import numpy as np
from jax import lax

D = 8192
KV = 512
BLOCK = 128
TOK_DEV = 640
GROUP_TOKENS = 40960
GROUPS = 4
N_GROUP = 4
N_FSDP = 64


def spiked(result, own_key, source, target, parts, factor):
    def block_of(axis_at):
        return (jnp.arange(result.shape[axis_at]) // (result.shape[axis_at] // parts)).reshape((-1,) + (1,) * (result.ndim - 1 - axis_at))

    one_side = jax.random.permutation(own_key, parts)[block_of(target)]
    far = (block_of(target) + parts // 2) % parts
    return jnp.where((block_of(source) == one_side) | (block_of(source) == far), factor * result, result)


def steps_of(stream_key, extent, shards, least, top_value):
    loudness, own = 1.0, jax.random.fold_in(stream_key, 6)
    for position, shards_of in shards:
        heights = jnp.exp(jax.random.uniform(jax.random.fold_in(own, position), (shards_of,), jnp.float32, least / len(shards), top_value / len(shards)))
        loudness = loudness * jnp.repeat(heights, extent[position] // shards_of).reshape([-1 if axis == position else 1 for axis in range(len(extent))])
    return loudness


def centred(key, extent, deviation, reach, cuts=(), held_as=jnp.bfloat16):
    result = deviation * jax.random.normal(key, extent, jnp.float32)
    if cuts:
        result = result * steps_of(key, extent, cuts, -0.22, 0.18)
    return jnp.clip(result, -reach, reach).astype(held_as)


def gaussian_with(key, shape, deviation, reach, pieces, heavy, held_as=jnp.bfloat16):
    drawn = deviation * jax.random.normal(key, shape, jnp.float32)
    if pieces:
        drawn = drawn * steps_of(key, shape, pieces, -0.22, 0.18)
    return jnp.clip(spiked(drawn, jax.random.fold_in(key, 3), *heavy), -reach, reach).astype(held_as)


def setup_inputs(seed: int = 0) -> dict:
    key_list = jax.random.split(jax.random.key(seed), 6)
    tokens = gaussian_with(key_list[0], (GROUPS, GROUP_TOKENS, D), 1.0, 16.0, ((0, 4), (1, 64)), (1, 2, 64, 4.0))
    keys_grad = centred(key_list[1], (GROUPS, GROUP_TOKENS, KV), 1.0, 6.0, ((0, 4), (1, 64)))
    norm_gain = jnp.clip(1.0 + 0.1 * jax.random.normal(key_list[2], (D,), jnp.float32), 0.5, 1.5)
    weight = centred(key_list[3], (D, KV), 1.0, 6.0, ((0, 64),))
    momentum = centred(key_list[4], (D, KV), 1.0, 6.0, ((0, 64), (1, 4)), jnp.float32)
    return {"tokens": tokens, "keys_grad": keys_grad, "norm_gain": norm_gain, "weight": weight, "momentum": momentum}


norm_epsilon = 1e-05
scale_epsilon = 1e-06
inner_rate = 0.5
outer_rate = 0.7
momentum_decay = 0.9

def quantize(values):
    array_shape = values.shape
    blocks = values.reshape(array_shape[:-1] + (array_shape[-1] // BLOCK, BLOCK))
    scales = (lax.optimization_barrier(jnp.max(jnp.abs(blocks), axis=-1)) + scale_epsilon).astype(jnp.bfloat16)
    payload = (blocks / scales.astype(jnp.float32)[..., None]).astype(jnp.bfloat16)
    return (payload.reshape(array_shape), scales)

def dequantize(payload, scales):
    array_shape = payload.shape
    blocks = payload.astype(jnp.float32).reshape(array_shape[:-1] + (array_shape[-1] // BLOCK, BLOCK))
    return (blocks * scales.astype(jnp.float32)[..., None]).reshape(array_shape)

def reference(tokens, keys_grad, norm_gain, weight, momentum):

    def group_delta(inputs):
        group_tokens, group_grads = inputs
        blocks_x = group_tokens.reshape(N_FSDP, TOK_DEV, D)
        blocks_g = group_grads.reshape(N_FSDP, TOK_DEV, KV)

        def accumulate(running_sum, block_pair):
            token_rows, cotangent = block_pair
            floats = token_rows.astype(jnp.float32)
            meansq = lax.optimization_barrier(jnp.mean(floats * floats, axis=1, keepdims=True))
            normed = (floats * lax.rsqrt(meansq + norm_epsilon) * norm_gain).astype(jnp.bfloat16)
            product = lax.dot_general(normed, cotangent, (((0,), (0,)), ((), ())), preferred_element_type=jnp.float32)
            return (running_sum + product, None)
        running_sum, unused = lax.scan(accumulate, jnp.zeros((D, KV), jnp.float32), (blocks_x, blocks_g))
        return running_sum * (inner_rate / math.sqrt(GROUP_TOKENS))
    deltas = lax.map(group_delta, (tokens, keys_grad))
    payload, scales = quantize(deltas)
    levels = N_GROUP.bit_length() - 1
    for section_index in range(levels):
        bit_index = levels - 1 - section_index
        partner = np.arange(N_GROUP) ^ 1 << bit_index
        values = dequantize(payload, scales)
        payload, scales = quantize(values + values[partner])
    average = dequantize(payload[0], scales[0]) / N_GROUP
    new_momentum = momentum_decay * momentum + average
    new_weight = (weight.astype(jnp.float32) - outer_rate * (average + momentum_decay * new_momentum)).astype(jnp.bfloat16)
    return (new_weight, new_momentum)
```

```python
import functools
import math

import jax
import jax.numpy as jnp
from jax import lax
from jax.experimental import pallas as pl
from jax.experimental.pallas import tpu as pltpu
from jax.sharding import Mesh
from jax.sharding import PartitionSpec as P

BLOCK = 128
ROWS_AT_A_TIME = 64
FSDP = ("x", "zl", "y")
GROUP = ("zh", "core")

norm_epsilon = 1e-05
inner_rate = 0.5
outer_rate = 0.7
momentum_decay = 0.9


def shift(block, axis, step):
    count = lax.axis_size(axis)
    return lax.ppermute(block, axis, [(i, (i + step) % count) for i in range(count)])


def swap(block, axis):
    return lax.ppermute(block, axis, [(0, 1), (1, 0)])


def wide(array):
    return array.astype(jnp.float32)


def narrow(array):
    return array.astype(jnp.bfloat16)


def products(first, place, grads, gain, tokens, send, own, stage, sems, column_of):
    x, zl, y = place[0], place[1], place[2]

    def out(ref, half, low, step):
        return pltpu.make_async_copy(stage.at[half, low, step], ref.at[low, step], sems.at[half])

    def body(turn, carry):
        low, step = turn // 4, turn % 4
        column = column_of(turn, lax.rem(x + step, 4), lax.rem(zl + first + low, 4))
        gain_at = (lax.rem(x + step, 4) * 4 + lax.rem(zl + first + low, 4)) * 4 * BLOCK
        tile = tokens[:, pl.ds(pl.multiple_of(column, BLOCK), 4 * BLOCK)]
        full = jnp.dot(grads[...], tile, preferred_element_type=jnp.float32)
        full = full * gain[:, pl.ds(pl.multiple_of(gain_at, BLOCK), 4 * BLOCK)]
        full = full.astype(jnp.bfloat16)
        for k in range(4):
            at = lax.rem(k + 4 - y, 4)
            for half in range(2):
                stage[half, low, step, at] = full[
                    half * 2 * BLOCK : (half + 1) * 2 * BLOCK, k * BLOCK : (k + 1) * BLOCK
                ]
        out(send, 0, low, step).start()
        out(own, 1, low, step).start()
        return carry

    lax.fori_loop(0, 8, body, 0)

    def drain(turn, carry):
        out(send, 0, turn // 4, turn % 4).wait()
        out(own, 1, turn // 4, turn % 4).wait()
        return carry

    lax.fori_loop(0, 8, drain, 0)


def first_kernel(factor, place, tokens, keys, gain, send, own, grads, held, scaled, stage, load, sems):
    count = held.shape[0] // ROWS_AT_A_TIME

    def rows(i):
        return pl.ds(pl.multiple_of(i * ROWS_AT_A_TIME, ROWS_AT_A_TIME), ROWS_AT_A_TIME)

    def read(i):
        return pltpu.make_async_copy(tokens.at[rows(i)], held.at[rows(i)], load.at[i])

    for i in range(count):
        read(i).start()

    def squares(i, carry):
        read(i).wait()
        total = jnp.zeros((ROWS_AT_A_TIME, BLOCK), jnp.float32)

        def add(j, total):
            for k in range(8):
                part = held[rows(i), pl.ds(pl.multiple_of((j * 8 + k) * BLOCK, BLOCK), BLOCK)].astype(jnp.float32)
                total = total + part * part
            return total

        total = lax.fori_loop(0, held.shape[1] // (8 * BLOCK), add, total)
        meansq = jnp.sum(total, axis=1, keepdims=True) / held.shape[1]
        scale = lax.rsqrt(meansq + norm_epsilon) * factor
        scaled[rows(i)] = keys[rows(i)].astype(jnp.float32) * scale
        return carry

    lax.fori_loop(0, count, squares, 0)

    core = place[3]
    for group in range(4):
        mine = jnp.where(core == group % 2, 2, 0)
        at = pl.ds(pl.multiple_of((mine + group // 2) * BLOCK, BLOCK), BLOCK)
        for t in range(held.shape[0] // BLOCK):
            square = scaled[t * BLOCK : (t + 1) * BLOCK, group * BLOCK : (group + 1) * BLOCK]
            grads[at, t * BLOCK : (t + 1) * BLOCK] = square.T.astype(jnp.bfloat16)

    def column_of(turn, x, zl):
        return (x * 4 + zl) * 4 * BLOCK

    products(0, place, grads, gain, held, send, own, stage, sems, column_of)


def second_kernel(place, tokens, grads, gain, send, own, held, stage, load, sems):
    def read(turn):
        x, zl = lax.rem(place[0] + turn % 4, 4), lax.rem(place[1] + 2 + turn // 4, 4)
        column = pl.multiple_of((x * 4 + zl) * 4 * BLOCK, 4 * BLOCK)
        to = pl.ds(pl.multiple_of(turn * 4 * BLOCK, 4 * BLOCK), 4 * BLOCK)
        return pltpu.make_async_copy(tokens.at[:, pl.ds(column, 4 * BLOCK)], held.at[:, to], load.at[turn])

    for turn in range(8):
        read(turn).start()

    def column_of(turn, x, zl):
        read(turn).wait()
        return turn * 4 * BLOCK

    products(2, place, grads, gain, held, send, own, stage, sems, column_of)


def gradient_terms(place, tokens, keys, gain, factor):
    count, width = tokens.shape
    cols = keys.shape[1]
    part = jax.ShapeDtypeStruct((2, 4, 4, cols // 2, BLOCK), jnp.bfloat16)
    any_space = pl.BlockSpec(memory_space=pl.ANY)
    in_vmem = pl.BlockSpec(memory_space=pltpu.VMEM)
    in_smem = pl.BlockSpec(memory_space=pltpu.SMEM)
    half = count * width * cols
    cost = pl.CostEstimate(flops=half, bytes_accessed=2 * count * width, transcendentals=0)
    stage = pltpu.VMEM((2, 2, 4, 4, cols // 2, BLOCK), jnp.bfloat16)
    send_a, own_a, grads = pl.pallas_call(
        functools.partial(first_kernel, factor),
        out_shape=[part, part, jax.ShapeDtypeStruct((cols, count), jnp.bfloat16)],
        in_specs=[in_smem, any_space, in_vmem, in_vmem],
        out_specs=[any_space, any_space, in_vmem],
        scratch_shapes=[
            pltpu.VMEM((count, width), jnp.bfloat16),
            pltpu.VMEM((count, cols), jnp.float32),
            stage,
            pltpu.SemaphoreType.DMA((count // ROWS_AT_A_TIME,)),
            pltpu.SemaphoreType.DMA((2,)),
        ],
        cost_estimate=cost,
        compiler_params=pltpu.CompilerParams(vmem_limit_bytes=56 * 2**20),
    )(place, tokens, keys, gain)
    send_b, own_b = pl.pallas_call(
        second_kernel,
        out_shape=[part, part],
        in_specs=[in_smem, any_space, in_vmem, in_vmem],
        out_specs=[any_space, any_space],
        scratch_shapes=[
            pltpu.VMEM((count, width // 2), jnp.bfloat16),
            stage,
            pltpu.SemaphoreType.DMA((8,)),
            pltpu.SemaphoreType.DMA((2,)),
        ],
        cost_estimate=cost,
        compiler_params=pltpu.CompilerParams(vmem_limit_bytes=56 * 2**20),
    )(place, tokens, grads, gain)
    return (send_a, own_a), (send_b, own_b)


def ring_sums(low, high, axis):
    far_low = shift(narrow(low(2)), axis, 1)
    far_high = shift(narrow(high(2)), axis, -1)
    up_high = shift(narrow(high(1)), axis, 1)
    down_low = shift(narrow(low(3)), axis, -1)
    up_low = shift(narrow(low(1) + wide(far_low)), axis, 1)
    down_high = shift(narrow(high(3) + wide(far_high)), axis, -1)
    return (
        low(0) + wide(down_low) + wide(up_low),
        high(0) + wide(up_high) + wide(down_high),
    )


def plane_sums(send, own, axes):
    received = swap(send, "core")

    def pair(which):
        at = (lambda s: (which, s)) if axes[0] == "x" else (lambda s: (which, slice(None), s))
        return lambda s: wide(own[at(s)]) + wide(received[at(s)])

    low, high = ring_sums(pair(0), pair(1), axes[0])
    return ring_sums(lambda s: low[s], lambda s: high[s], axes[1])


def per_device(tokens, keys_grad, norm_gain, weight, momentum):
    x, zl, y, zh, core = (lax.axis_index(a) for a in FSDP + GROUP)
    rows, cols = momentum.shape

    pair = jnp.stack([momentum, swap(momentum, "zh")])
    pair = jnp.where(zh == 0, pair, pair[::-1])
    both = jnp.stack([pair, swap(pair, "core")])
    both = jnp.where(core == 0, both, both[::-1])

    groups = lax.axis_size(GROUP)
    factor = inner_rate / math.sqrt(lax.axis_size(FSDP) * tokens.shape[1]) / groups
    place = jnp.stack([x, zl, y, core]).astype(jnp.int32)
    part_a, part_b = gradient_terms(place, tokens[0], keys_grad[0], norm_gain[None, :], factor)

    lines = plane_sums(*part_a, ("x", "y")) + plane_sums(*part_b, ("y", "x"))
    partial = lines[0]
    for step in (1, 2, 3):
        partial += wide(shift(narrow(lines[step]), "zl", step))

    rounded = narrow(partial)
    average = wide(rounded) + wide(swap(rounded, "zh"))
    average = average.reshape(2, cols, rows)
    averages = jnp.stack([average, swap(average, "core")])
    averages = jnp.where(core == 0, averages, averages[::-1])

    own_average = jnp.where(zh == 0, average[0], average[1])
    new_momentum = momentum_decay * momentum + own_average.T
    averages = averages.transpose(3, 1, 0, 2).reshape(rows, 4 * cols)
    both = both.transpose(2, 1, 0, 3).reshape(rows, 4 * cols)
    update = averages + momentum_decay * (momentum_decay * both + averages)
    new_weight = (wide(weight) - outer_rate * update).astype(jnp.bfloat16)
    return (new_weight, new_momentum)


def solution(mesh):
    finer = Mesh(mesh.devices.reshape(2, 2, 4, 4, 4), GROUP + FSDP)
    in_specs = (
        P(GROUP, FSDP, None),
        P(GROUP, FSDP, None),
        P(),
        P(FSDP, None),
        P(FSDP, GROUP),
    )
    out_specs = (P(FSDP, None), P(FSDP, GROUP))
    return jax.shard_map(
        per_device, mesh=finer, in_specs=in_specs, out_specs=out_specs, check_vma=False
    )
```

```python
import functools
import math

import jax
import jax.numpy as jnp
from jax import lax
from jax.experimental import pallas as pl
from jax.experimental.pallas import tpu as pltpu
from jax.sharding import Mesh
from jax.sharding import PartitionSpec as P


BLOCK = 128
ROWS_AT_A_TIME = 64
FSDP = ("x", "zl", "y")
GROUP = ("zh", "core")

norm_epsilon = 1e-05
inner_rate = 0.5
outer_rate = 0.7
momentum_decay = 0.9


def shift(block, axis, step):
    count = lax.axis_size(axis)
    return lax.ppermute(block, axis, [(i, (i + step) % count) for i in range(count)])


def onward(block, axis, step):
    route = [(i, (i + step) % 4) for i in range(4)] + [(4 + i, 4 + (i - step) % 4) for i in range(4)]
    return lax.ppermute(block, ("core", axis), route)


def swap(block, axis):
    return lax.ppermute(block, axis, [(0, 1), (1, 0)])


def wide(array):
    return array.astype(jnp.float32)


def narrow(array):
    return array.astype(jnp.bfloat16)


class Tiles:
    def __init__(self, place, distances):
        self.x, self.zl, self.y, self.core = (place[i] for i in range(4))
        self.distances = distances
        self.count = 4 * len(distances)

    def parts(self, turn):
        return turn // 4, (turn // 2) % 2, turn % 2

    def column(self, turn, block):
        at, colour, low = self.parts(turn)
        distance = self.distances[0] + 2 * at
        along = jnp.where(colour == 0, self.x, self.y)
        along = lax.rem(along + 4 + jnp.where(self.core == 0, distance, -distance), 4)
        line = lax.rem(self.zl + 2 * colour + low, 4)
        x, y = jnp.where(colour == 0, along, block), jnp.where(colour == 0, block, along)
        return pl.multiple_of(((x * 4 + line) * 4 + y) * BLOCK, BLOCK)

    def second(self, colour, block):
        across = jnp.where(colour == 0, self.y, self.x)
        return lax.rem(jnp.where(self.core == 0, block - across, across - block) + 4, 4)

    def products(self, grads, gain, tile_of, send, own, stage, sems):
        def out(turn, half):
            at, colour, low = self.parts(turn)
            if half == 0:
                at = len(self.distances) - 1 - at
            ref = (send, own)[half]
            return pltpu.make_async_copy(
                stage.at[half, at, colour, :, low], ref.at[at, colour, :, low], sems.at[half]
            )

        def body(turn, carry):
            at, colour, low = self.parts(turn)
            tile = tile_of(turn)
            full = jnp.dot(grads[...], tile, preferred_element_type=jnp.float32)
            rows = full.shape[0] // 2
            for k in range(4):
                scale = gain[:, pl.ds(self.column(turn, k), BLOCK)]
                block = (full[:, k * BLOCK : (k + 1) * BLOCK] * scale).astype(jnp.bfloat16)
                there = self.second(colour, k)
                stage[0, len(self.distances) - 1 - at, colour, lax.rem(4 - there, 4), low] = block[:rows]
                stage[1, at, colour, there, low] = block[rows:]
            out(turn, 0).start()
            out(turn, 1).start()
            return carry

        lax.fori_loop(0, self.count, body, 0)

        def drain(turn, carry):
            out(turn, 0).wait()
            out(turn, 1).wait()
            return carry

        lax.fori_loop(0, self.count, drain, 0)


def first_kernel(factor, place, tokens, keys, gain, send, own, grads, held, scaled, stage, load, sems):
    count = held.shape[0] // ROWS_AT_A_TIME

    def rows(i):
        return pl.ds(pl.multiple_of(i * ROWS_AT_A_TIME, ROWS_AT_A_TIME), ROWS_AT_A_TIME)

    def read(i):
        return pltpu.make_async_copy(tokens.at[rows(i)], held.at[rows(i)], load.at[i])

    for i in range(count):
        read(i).start()

    def squares(i, carry):
        read(i).wait()
        total = jnp.zeros((ROWS_AT_A_TIME, BLOCK), jnp.float32)

        def add(j, total):
            for k in range(8):
                part = held[rows(i), pl.ds(pl.multiple_of((j * 8 + k) * BLOCK, BLOCK), BLOCK)].astype(jnp.float32)
                total = total + part * part
            return total

        total = lax.fori_loop(0, held.shape[1] // (8 * BLOCK), add, total)
        meansq = jnp.sum(total, axis=1, keepdims=True) / held.shape[1]
        scale = lax.rsqrt(meansq + norm_epsilon) * factor
        scaled[rows(i)] = keys[rows(i)].astype(jnp.float32) * scale
        return carry

    lax.fori_loop(0, count, squares, 0)

    core = place[3]
    for group in range(4):
        mine = jnp.where(core == group % 2, 2, 0)
        at = pl.ds(pl.multiple_of((mine + group // 2) * BLOCK, BLOCK), BLOCK)
        for t in range(held.shape[0] // BLOCK):
            square = scaled[t * BLOCK : (t + 1) * BLOCK, group * BLOCK : (group + 1) * BLOCK]
            grads[at, t * BLOCK : (t + 1) * BLOCK] = square.T.astype(jnp.bfloat16)

    tiles = Tiles(place, (2,))

    def tile_of(turn):
        return jnp.concatenate([held[:, pl.ds(tiles.column(turn, k), BLOCK)] for k in range(4)], axis=1)

    tiles.products(grads, gain, tile_of, send, own, stage, sems)


def later_kernel(distances, place, tokens, grads, gain, send, own, held, stage, load, sems):
    tiles = Tiles(place, distances)

    def read(turn, k):
        return pltpu.make_async_copy(
            tokens.at[:, pl.ds(tiles.column(turn, k), BLOCK)],
            held.at[turn, :, k * BLOCK : (k + 1) * BLOCK],
            load.at[turn, k],
        )

    for turn in range(tiles.count):
        for k in range(4):
            read(turn, k).start()

    def tile_of(turn):
        for k in range(4):
            read(turn, k).wait()
        return held[turn]

    tiles.products(grads, gain, tile_of, send, own, stage, sems)


def first_terms(place, tokens, keys, gain, factor):
    count, width = tokens.shape
    cols = keys.shape[1]
    part = jax.ShapeDtypeStruct((1, 2, 4, 2, cols // 2, BLOCK), jnp.bfloat16)
    any_space = pl.BlockSpec(memory_space=pl.ANY)
    in_vmem = pl.BlockSpec(memory_space=pltpu.VMEM)
    in_smem = pl.BlockSpec(memory_space=pltpu.SMEM)
    return pl.pallas_call(
        functools.partial(first_kernel, factor),
        out_shape=[part, part, jax.ShapeDtypeStruct((cols, count), jnp.bfloat16)],
        in_specs=[in_smem, any_space, in_vmem, in_vmem],
        out_specs=[any_space, any_space, in_vmem],
        scratch_shapes=[
            pltpu.VMEM((count, width), jnp.bfloat16),
            pltpu.VMEM((count, cols), jnp.float32),
            pltpu.VMEM((2,) + part.shape, jnp.bfloat16),
            pltpu.SemaphoreType.DMA((count // ROWS_AT_A_TIME,)),
            pltpu.SemaphoreType.DMA((2,)),
        ],
        cost_estimate=pl.CostEstimate(
            flops=count * width * cols // 2, bytes_accessed=2 * count * width, transcendentals=0
        ),
        compiler_params=pltpu.CompilerParams(vmem_limit_bytes=56 * 2**20),
    )(place, tokens, keys, gain)


def later_terms(distances, place, tokens, grads, gain):
    count, width = tokens.shape
    cols = grads.shape[0]
    part = jax.ShapeDtypeStruct((len(distances), 2, 4, 2, cols // 2, BLOCK), jnp.bfloat16)
    any_space = pl.BlockSpec(memory_space=pl.ANY)
    in_vmem = pl.BlockSpec(memory_space=pltpu.VMEM)
    in_smem = pl.BlockSpec(memory_space=pltpu.SMEM)
    turns = 4 * len(distances)
    return pl.pallas_call(
        functools.partial(later_kernel, distances),
        out_shape=[part, part],
        in_specs=[in_smem, any_space, in_vmem, in_vmem],
        out_specs=[any_space, any_space],
        scratch_shapes=[
            pltpu.VMEM((turns, count, 4 * BLOCK), jnp.bfloat16),
            pltpu.VMEM((2,) + part.shape, jnp.bfloat16),
            pltpu.SemaphoreType.DMA((turns, 4)),
            pltpu.SemaphoreType.DMA((2,)),
        ],
        cost_estimate=pl.CostEstimate(
            flops=2 * turns * count * cols * 4 * BLOCK, bytes_accessed=2 * count * width, transcendentals=0
        ),
        compiler_params=pltpu.CompilerParams(vmem_limit_bytes=52 * 2**20),
    )(place, tokens, grads, gain)


def ring_sum(terms, axis):
    far = onward(narrow(terms[2]), axis, 1)
    back = onward(narrow(terms[3]), axis, -1)
    front = onward(narrow(terms[1] + wide(far)), axis, 1)
    return terms[0] + wide(back) + wide(front)


def per_device(tokens, keys_grad, norm_gain, weight, momentum):
    x, zl, y, zh, core = (lax.axis_index(a) for a in FSDP + GROUP)
    rows, cols = momentum.shape
    groups = lax.axis_size(GROUP)
    factor = inner_rate / math.sqrt(lax.axis_size(FSDP) * tokens.shape[1]) / groups
    place = jnp.stack([x, zl, y, core]).astype(jnp.int32)
    gain = norm_gain[None, :]
    axes = ("x", "y")

    send, own, grads = first_terms(place, tokens[0], keys_grad[0], gain, factor)
    received = swap(send, "core")
    far = [None, None]
    for c in (0, 1):
        far[c] = onward(narrow(wide(own[0, c]) + wide(received[0, c])), axes[c], 1)

    send, own = later_terms((1, 3), place, tokens[0], grads, gain)
    received = swap(send, "core")
    sides = [[wide(own[i, c]) + wide(received[i, c]) for i in (0, 1)] for c in (0, 1)]
    back = [None, None]
    for c in (0, 1):
        back[c] = onward(narrow(sides[c][1]), axes[c], -1)

    send, own = later_terms((0,), place, tokens[0], grads, gain)
    received = swap(send, "core")
    front = [onward(narrow(sides[c][0] + wide(far[c])), axes[c], 1) for c in (0, 1)]
    sums = [wide(own[0, c]) + wide(received[0, c]) + wide(back[c]) + wide(front[c]) for c in (0, 1)]

    sums = [ring_sum(sums[0], "y"), ring_sum(sums[1], "x")]
    lines = [sums[0][0], sums[0][1], sums[1][0], sums[1][1]]
    partial = lines[0]
    for step in (1, 2, 3):
        partial += wide(shift(narrow(lines[step]), "zl", step))

    partial = partial.reshape(2, cols, rows)
    both_rate = 1 + momentum_decay
    mine = (jnp.arange(2) == zh)[:, None, None]
    joined = narrow(partial + jnp.where(mine, momentum.T * (momentum_decay**2 / both_rate), 0.0))
    received = swap(joined, "zh")
    update = wide(joined) + wide(received)
    updates = jnp.stack([update, swap(update, "core")])
    updates = jnp.where(core == 0, updates, updates[::-1])
    average = jnp.where(zh == 0, partial[0] + wide(received[0]), partial[1] + wide(received[1]))

    new_momentum = momentum_decay * momentum + average.T
    updates = updates.transpose(3, 1, 0, 2).reshape(rows, 4 * cols)
    new_weight = narrow(wide(weight) - outer_rate * both_rate * updates)
    return (new_weight, new_momentum)


def solution(mesh):
    finer = Mesh(mesh.devices.reshape(2, 2, 4, 4, 4), GROUP + FSDP)
    in_specs = (
        P(GROUP, FSDP, None),
        P(GROUP, FSDP, None),
        P(),
        P(FSDP, None),
        P(FSDP, GROUP),
    )
    out_specs = (P(FSDP, None), P(FSDP, GROUP))
    return jax.shard_map(per_device, mesh=finer, in_specs=in_specs, out_specs=out_specs, check_vma=False)
```

```python
import functools
import math

import jax
import jax.numpy as jnp
from jax import lax
from jax.experimental import pallas as pl
from jax.experimental.pallas import tpu as pltpu
from jax.sharding import Mesh
from jax.sharding import PartitionSpec as P


BLOCK = 128
ROWS_AT_A_TIME = 64
VMEM_LIMIT = 24 * 2**20
FSDP = ("x", "zl", "y")
GROUP = ("zh", "core")

norm_epsilon = 1e-05
inner_rate = 0.5
outer_rate = 0.7
momentum_decay = 0.9


def shift(block, axis, step):
    count = lax.axis_size(axis)
    return lax.ppermute(block, axis, [(i, (i + step) % count) for i in range(count)])


def onward(block, axis, step):
    route = [(i, (i + step) % 4) for i in range(4)] + [(4 + i, 4 + (i - step) % 4) for i in range(4)]
    return lax.ppermute(block, ("core", axis), route)


def swap(block, axis):
    return lax.ppermute(block, axis, [(0, 1), (1, 0)])


def wide(array):
    return array.astype(jnp.float32)


def narrow(array):
    return array.astype(jnp.bfloat16)


class Tiles:
    def __init__(self, place, distances):
        self.x, self.zl, self.y, self.core = (place[i] for i in range(4))
        self.distances = distances
        self.count = 4 * len(distances)

    def parts(self, turn):
        return turn // 4, (turn // 2) % 2, turn % 2

    def column(self, turn, block):
        at, colour, low = self.parts(turn)
        distance = self.distances[0] + 2 * at
        along = jnp.where(colour == 0, self.x, self.y)
        along = lax.rem(along + 4 + jnp.where(self.core == 0, distance, -distance), 4)
        line = lax.rem(self.zl + 2 * colour + low, 4)
        x, y = jnp.where(colour == 0, along, block), jnp.where(colour == 0, block, along)
        return pl.multiple_of(((x * 4 + line) * 4 + y) * BLOCK, BLOCK)

    def second(self, colour, block):
        across = jnp.where(colour == 0, self.y, self.x)
        return lax.rem(jnp.where(self.core == 0, block - across, across - block) + 4, 4)

    def products(self, tokens, grads, gain, send, own):
        def body(turn, carry):
            at, colour, low = self.parts(turn)
            columns = [pl.ds(self.column(turn, k), BLOCK) for k in range(4)]
            tile = jnp.concatenate([tokens[:, c] for c in columns], axis=1)
            full = jnp.dot(grads[...], tile, preferred_element_type=jnp.float32)
            rows = full.shape[0] // 2
            for k in range(4):
                block = (full[:, k * BLOCK : (k + 1) * BLOCK] * gain[:, columns[k]]).astype(jnp.bfloat16)
                there = self.second(colour, k)
                send[len(self.distances) - 1 - at, colour, lax.rem(4 - there, 4), low] = block[:rows]
                own[at, colour, there, low] = block[rows:]
            return carry

        lax.fori_loop(0, self.count, body, 0)


def first_kernel(factor, place, tokens, keys, gain, send, own, grads, scaled):
    count, width = tokens.shape

    def squares(i, carry):
        rows = pl.ds(pl.multiple_of(i * ROWS_AT_A_TIME, ROWS_AT_A_TIME), ROWS_AT_A_TIME)

        def add(j, total):
            for k in range(8):
                part = tokens[rows, pl.ds(pl.multiple_of((j * 8 + k) * BLOCK, BLOCK), BLOCK)].astype(jnp.float32)
                total = total + part * part
            return total

        total = jnp.zeros((ROWS_AT_A_TIME, BLOCK), jnp.float32)
        total = lax.fori_loop(0, width // (8 * BLOCK), add, total)
        meansq = jnp.sum(total, axis=1, keepdims=True) / width
        scale = lax.rsqrt(meansq + norm_epsilon) * factor
        scaled[rows] = keys[rows].astype(jnp.float32) * scale
        return carry

    lax.fori_loop(0, count // ROWS_AT_A_TIME, squares, 0)

    core = place[3]
    for group in range(4):
        mine = jnp.where(core == group % 2, 2, 0)
        at = pl.ds(pl.multiple_of((mine + group // 2) * BLOCK, BLOCK), BLOCK)
        for t in range(count // BLOCK):
            square = scaled[t * BLOCK : (t + 1) * BLOCK, group * BLOCK : (group + 1) * BLOCK]
            grads[at, t * BLOCK : (t + 1) * BLOCK] = square.T.astype(jnp.bfloat16)

    Tiles(place, (2,)).products(tokens, grads, gain, send, own)


def later_kernel(distances, place, tokens, grads, gain, send, own):
    Tiles(place, distances).products(tokens, grads, gain, send, own)


def terms(kernel, distances, outs, scratch, place, tokens, grads, gain):
    count = tokens.shape[0]
    cols = 4 * BLOCK
    part = jax.ShapeDtypeStruct((len(distances), 2, 4, 2, cols // 2, BLOCK), jnp.bfloat16)
    in_vmem = pl.BlockSpec(memory_space=pltpu.VMEM)
    in_smem = pl.BlockSpec(memory_space=pltpu.SMEM)
    outs = [part, part] + outs
    flops = 2 * len(distances) * 16 * BLOCK * count * cols
    return pl.pallas_call(
        kernel,
        out_shape=outs,
        in_specs=[in_smem, in_vmem, in_vmem, in_vmem],
        out_specs=[in_vmem] * len(outs),
        scratch_shapes=scratch,
        cost_estimate=pl.CostEstimate(flops=flops, bytes_accessed=2**20, transcendentals=0),
        compiler_params=pltpu.CompilerParams(vmem_limit_bytes=VMEM_LIMIT),
    )(place, tokens, grads, gain)


def first_terms(place, tokens, keys, gain, factor):
    count, cols = keys.shape
    grads = jax.ShapeDtypeStruct((cols, count), jnp.bfloat16)
    scratch = [pltpu.VMEM((count, cols), jnp.float32)]
    return terms(functools.partial(first_kernel, factor), (2,), [grads], scratch, place, tokens, keys, gain)


def later_terms(distances, place, tokens, grads, gain):
    return terms(functools.partial(later_kernel, distances), distances, [], [], place, tokens, grads, gain)


def ring_sum(terms, axis):
    far = onward(narrow(terms[2]), axis, 1)
    back = onward(narrow(terms[3]), axis, -1)
    front = onward(narrow(terms[1] + wide(far)), axis, 1)
    return terms[0] + wide(back) + wide(front)


def per_device(tokens, keys_grad, norm_gain, weight, momentum):
    x, zl, y, zh, core = (lax.axis_index(a) for a in FSDP + GROUP)
    rows, cols = momentum.shape
    groups = lax.axis_size(GROUP)
    factor = inner_rate / math.sqrt(lax.axis_size(FSDP) * tokens.shape[1]) / groups
    place = jnp.stack([x, zl, y, core]).astype(jnp.int32)
    gain = norm_gain[None, :]
    axes = ("x", "y")

    send, own, grads = first_terms(place, tokens[0], keys_grad[0], gain, factor)
    received = swap(send, "core")
    far = [None, None]
    for c in (0, 1):
        far[c] = onward(narrow(wide(own[0, c]) + wide(received[0, c])), axes[c], 1)

    send, own = later_terms((1, 3), place, tokens[0], grads, gain)
    received = swap(send, "core")
    sides = [[wide(own[i, c]) + wide(received[i, c]) for i in (0, 1)] for c in (0, 1)]
    back = [None, None]
    for c in (0, 1):
        back[c] = onward(narrow(sides[c][1]), axes[c], -1)

    front = [None, None]
    for c in (0, 1):
        front[c] = onward(narrow(sides[c][0] + wide(far[c])), axes[c], 1)

    send, own = later_terms((0,), place, tokens[0], grads, gain)
    received = swap(send, "core")
    sums = [wide(own[0, c]) + wide(received[0, c]) + wide(back[c]) + wide(front[c]) for c in (0, 1)]

    sums = [ring_sum(sums[0], "y"), ring_sum(sums[1], "x")]
    lines = [sums[0][0], sums[0][1], sums[1][0], sums[1][1]]
    partial = lines[0]
    for step in (1, 2, 3):
        partial += wide(shift(narrow(lines[step]), "zl", step))

    partial = partial.reshape(2, cols, rows)
    both_rate = 1 + momentum_decay
    mine = (jnp.arange(2) == zh)[:, None, None]
    joined = narrow(partial + jnp.where(mine, momentum.T * (momentum_decay**2 / both_rate), 0.0))
    received = swap(joined, "zh")
    update = wide(joined) + wide(received)
    updates = jnp.stack([update, swap(update, "core")])
    updates = jnp.where(core == 0, updates, updates[::-1])
    average = jnp.where(zh == 0, partial[0] + wide(received[0]), partial[1] + wide(received[1]))

    new_momentum = momentum_decay * momentum + average.T
    updates = updates.transpose(3, 1, 0, 2).reshape(rows, 4 * cols)
    new_weight = narrow(wide(weight) - outer_rate * both_rate * updates)
    return (new_weight, new_momentum)


def solution(mesh):
    finer = Mesh(mesh.devices.reshape(2, 2, 4, 4, 4), GROUP + FSDP)
    in_specs = (
        P(GROUP, FSDP, None),
        P(GROUP, FSDP, None),
        P(),
        P(FSDP, None),
        P(FSDP, GROUP),
    )
    out_specs = (P(FSDP, None), P(FSDP, GROUP))
    return jax.shard_map(per_device, mesh=finer, in_specs=in_specs, out_specs=out_specs, check_vma=False)
```

```python
import functools
import math

import jax
import jax.numpy as jnp
from jax import lax
from jax.experimental import pallas as pl
from jax.experimental.pallas import tpu as pltpu
from jax.sharding import Mesh
from jax.sharding import PartitionSpec as P


BLOCK = 128
ROWS_AT_A_TIME = 64
FIRST_LIMIT = 38
LATER_LIMIT = 24
FSDP = ("x", "zl", "y")
GROUP = ("zh", "core")

norm_epsilon = 1e-05
inner_rate = 0.5
outer_rate = 0.7
momentum_decay = 0.9


def shift(block, axis, step):
    count = lax.axis_size(axis)
    return lax.ppermute(block, axis, [(i, (i + step) % count) for i in range(count)])


def onward(block, axis, step):
    route = [(i, (i + step) % 4) for i in range(4)] + [(4 + i, 4 + (i - step) % 4) for i in range(4)]
    return lax.ppermute(block, ("core", axis), route)


def swap(block, axis):
    return lax.ppermute(block, axis, [(0, 1), (1, 0)])


def wide(array):
    return array.astype(jnp.float32)


def narrow(array):
    return array.astype(jnp.bfloat16)


class Tiles:
    def __init__(self, place, distances):
        self.x, self.zl, self.y, self.core = (place[i] for i in range(4))
        self.distances = distances
        self.count = 4 * len(distances)

    def parts(self, turn):
        return turn // 4, (turn // 2) % 2, turn % 2

    def column(self, turn, block):
        at, colour, low = self.parts(turn)
        distance = self.distances[0] + 2 * at
        along = jnp.where(colour == 0, self.x, self.y)
        along = lax.rem(along + 4 + jnp.where(self.core == 0, distance, -distance), 4)
        line = lax.rem(self.zl + 2 * colour + low, 4)
        x, y = jnp.where(colour == 0, along, block), jnp.where(colour == 0, block, along)
        return pl.multiple_of(((x * 4 + line) * 4 + y) * BLOCK, BLOCK)

    def second(self, colour, block):
        across = jnp.where(colour == 0, self.y, self.x)
        return lax.rem(jnp.where(self.core == 0, block - across, across - block) + 4, 4)

    def products(self, tokens, grads, gain, send, own):
        def body(turn, carry):
            at, colour, low = self.parts(turn)
            columns = [pl.ds(self.column(turn, k), BLOCK) for k in range(4)]
            tile = jnp.concatenate([tokens[:, c] for c in columns], axis=1)
            full = jnp.dot(grads[...], tile, preferred_element_type=jnp.float32)
            rows = full.shape[0] // 2
            for k in range(4):
                block = (full[:, k * BLOCK : (k + 1) * BLOCK] * gain[:, columns[k]]).astype(jnp.bfloat16)
                there = self.second(colour, k)
                send[len(self.distances) - 1 - at, colour, lax.rem(4 - there, 4), low] = block[:rows]
                own[at, colour, there, low] = block[rows:]
            return carry

        lax.fori_loop(0, self.count, body, 0)


def first_kernel(factor, place, tokens, keys, gain, send, own, held, grads, scaled, load):
    count, width = tokens.shape

    def rows_of(i):
        return pl.ds(pl.multiple_of(i * ROWS_AT_A_TIME, ROWS_AT_A_TIME), ROWS_AT_A_TIME)

    def read(i):
        return pltpu.make_async_copy(tokens.at[rows_of(i)], held.at[rows_of(i)], load.at[i])

    for i in range(count // ROWS_AT_A_TIME):
        read(i).start()

    def squares(i, carry):
        read(i).wait()
        rows = rows_of(i)

        def add(j, total):
            for k in range(8):
                part = held[rows, pl.ds(pl.multiple_of((j * 8 + k) * BLOCK, BLOCK), BLOCK)].astype(jnp.float32)
                total = total + part * part
            return total

        total = jnp.zeros((ROWS_AT_A_TIME, BLOCK), jnp.float32)
        total = lax.fori_loop(0, width // (8 * BLOCK), add, total)
        meansq = jnp.sum(total, axis=1, keepdims=True) / width
        scale = lax.rsqrt(meansq + norm_epsilon) * factor
        scaled[rows] = keys[rows].astype(jnp.float32) * scale
        return carry

    lax.fori_loop(0, count // ROWS_AT_A_TIME, squares, 0)

    core = place[3]
    for group in range(4):
        mine = jnp.where(core == group % 2, 2, 0)
        at = pl.ds(pl.multiple_of((mine + group // 2) * BLOCK, BLOCK), BLOCK)
        for t in range(count // BLOCK):
            square = scaled[t * BLOCK : (t + 1) * BLOCK, group * BLOCK : (group + 1) * BLOCK]
            grads[at, t * BLOCK : (t + 1) * BLOCK] = square.T.astype(jnp.bfloat16)

    Tiles(place, (2,)).products(held, grads, gain, send, own)


def later_kernel(distances, place, tokens, grads, gain, send, own):
    Tiles(place, distances).products(tokens, grads, gain, send, own)


def terms(kernel, distances, outs, scratch, tokens_in, limit, place, tokens, grads, gain):
    count = tokens.shape[0]
    cols = 4 * BLOCK
    part = jax.ShapeDtypeStruct((len(distances), 2, 4, 2, cols // 2, BLOCK), jnp.bfloat16)
    in_vmem = pl.BlockSpec(memory_space=pltpu.VMEM)
    in_smem = pl.BlockSpec(memory_space=pltpu.SMEM)
    outs = [part, part] + outs
    flops = 2 * len(distances) * 16 * BLOCK * count * cols
    return pl.pallas_call(
        kernel,
        out_shape=outs,
        in_specs=[in_smem, pl.BlockSpec(memory_space=tokens_in), in_vmem, in_vmem],
        out_specs=[in_vmem] * len(outs),
        scratch_shapes=scratch,
        cost_estimate=pl.CostEstimate(flops=flops, bytes_accessed=2**20, transcendentals=0),
        compiler_params=pltpu.CompilerParams(vmem_limit_bytes=limit * 2**20),
    )(place, tokens, grads, gain)


def first_terms(place, tokens, keys, gain, factor):
    count, cols = keys.shape
    outs = [jax.ShapeDtypeStruct(tokens.shape, jnp.bfloat16), jax.ShapeDtypeStruct((cols, count), jnp.bfloat16)]
    scratch = [pltpu.VMEM((count, cols), jnp.float32), pltpu.SemaphoreType.DMA((count // ROWS_AT_A_TIME,))]
    kernel = functools.partial(first_kernel, factor)
    return terms(kernel, (2,), outs, scratch, pl.ANY, FIRST_LIMIT, place, tokens, keys, gain)


def later_terms(distances, place, tokens, grads, gain):
    kernel = functools.partial(later_kernel, distances)
    return terms(kernel, distances, [], [], pltpu.VMEM, LATER_LIMIT, place, tokens, grads, gain)


def ring_sum(terms, axis):
    far = onward(narrow(terms[2]), axis, 1)
    back = onward(narrow(terms[3]), axis, -1)
    front = onward(narrow(terms[1] + wide(far)), axis, 1)
    return terms[0] + wide(back) + wide(front)


def per_device(tokens, keys_grad, norm_gain, weight, momentum):
    x, zl, y, zh, core = (lax.axis_index(a) for a in FSDP + GROUP)
    rows, cols = momentum.shape
    groups = lax.axis_size(GROUP)
    factor = inner_rate / math.sqrt(lax.axis_size(FSDP) * tokens.shape[1]) / groups
    place = jnp.stack([x, zl, y, core]).astype(jnp.int32)
    gain = norm_gain[None, :]
    axes = ("x", "y")

    send, own, held, grads = first_terms(place, tokens[0], keys_grad[0], gain, factor)
    received = swap(send, "core")
    far = [None, None]
    for c in (0, 1):
        far[c] = onward(narrow(wide(own[0, c]) + wide(received[0, c])), axes[c], 1)

    send, own = later_terms((1, 3), place, held, grads, gain)
    received = swap(send, "core")
    sides = [[wide(own[i, c]) + wide(received[i, c]) for i in (0, 1)] for c in (0, 1)]
    back = [None, None]
    for c in (0, 1):
        back[c] = onward(narrow(sides[c][1]), axes[c], -1)

    front = [None, None]
    for c in (0, 1):
        front[c] = onward(narrow(sides[c][0] + wide(far[c])), axes[c], 1)

    send, own = later_terms((0,), place, held, grads, gain)
    received = swap(send, "core")
    sums = [wide(own[0, c]) + wide(received[0, c]) + wide(back[c]) + wide(front[c]) for c in (0, 1)]

    sums = [ring_sum(sums[0], "y"), ring_sum(sums[1], "x")]
    lines = [sums[0][0], sums[0][1], sums[1][0], sums[1][1]]
    partial = lines[0]
    for step in (1, 2, 3):
        partial += wide(shift(narrow(lines[step]), "zl", step))

    partial = partial.reshape(2, cols, rows)
    both_rate = 1 + momentum_decay
    mine = (jnp.arange(2) == zh)[:, None, None]
    joined = narrow(partial + jnp.where(mine, momentum.T * (momentum_decay**2 / both_rate), 0.0))
    received = swap(joined, "zh")
    update = wide(joined) + wide(received)
    updates = jnp.stack([update, swap(update, "core")])
    updates = jnp.where(core == 0, updates, updates[::-1])
    average = jnp.where(zh == 0, partial[0] + wide(received[0]), partial[1] + wide(received[1]))

    new_momentum = momentum_decay * momentum + average.T
    updates = updates.transpose(3, 1, 0, 2).reshape(rows, 4 * cols)
    new_weight = narrow(wide(weight) - outer_rate * both_rate * updates)
    return (new_weight, new_momentum)


def solution(mesh):
    finer = Mesh(mesh.devices.reshape(2, 2, 4, 4, 4), GROUP + FSDP)
    in_specs = (
        P(GROUP, FSDP, None),
        P(GROUP, FSDP, None),
        P(),
        P(FSDP, None),
        P(FSDP, GROUP),
    )
    out_specs = (P(FSDP, None), P(FSDP, GROUP))
    return jax.shard_map(per_device, mesh=finer, in_specs=in_specs, out_specs=out_specs, check_vma=False)
```

```python
import functools
import math

import jax
import jax.numpy as jnp
from jax import lax
from jax.experimental import pallas as pl
from jax.experimental.pallas import tpu as pltpu
from jax.sharding import Mesh
from jax.sharding import PartitionSpec as P


BLOCK = 128
ROWS_AT_A_TIME = 64
FIRST_LIMIT = 38
LATER_LIMIT = 24
FSDP = ("x", "zl", "y")
GROUP = ("zh", "core")

norm_epsilon = 1e-05
inner_rate = 0.5
outer_rate = 0.7
momentum_decay = 0.9


def shift(block, axis, step):
    count = lax.axis_size(axis)
    return lax.ppermute(block, axis, [(i, (i + step) % count) for i in range(count)])


def onward(block, axis, step):
    route = [(i, (i + step) % 4) for i in range(4)] + [(4 + i, 4 + (i - step) % 4) for i in range(4)]
    return lax.ppermute(block, ("core", axis), route)


def swap(block, axis):
    return lax.ppermute(block, axis, [(0, 1), (1, 0)])


def wide(array):
    return array.astype(jnp.float32)


def narrow(array):
    return array.astype(jnp.bfloat16)


class Tiles:
    def __init__(self, place, distances):
        self.x, self.zl, self.y, self.core = (place[i] for i in range(4))
        self.distances = distances
        self.count = 4 * len(distances)

    def parts(self, turn):
        return turn // 4, (turn // 2) % 2, turn % 2

    def column(self, turn, block):
        at, colour, low = self.parts(turn)
        distance = self.distances[0] + 2 * at
        along = jnp.where(colour == 0, self.x, self.y)
        along = lax.rem(along + 4 + jnp.where(self.core == 0, distance, -distance), 4)
        line = lax.rem(self.zl + 2 * colour + low, 4)
        x, y = jnp.where(colour == 0, along, block), jnp.where(colour == 0, block, along)
        return pl.multiple_of(((x * 4 + line) * 4 + y) * BLOCK, BLOCK)

    def second(self, colour, block):
        across = jnp.where(colour == 0, self.y, self.x)
        return lax.rem(jnp.where(self.core == 0, block - across, across - block) + 4, 4)

    def products(self, tokens, grads, gain, send, own):
        def body(turn, carry):
            at, colour, low = self.parts(turn)
            columns = [pl.ds(self.column(turn, k), BLOCK) for k in range(4)]
            tile = jnp.concatenate([tokens[:, c] for c in columns], axis=1)
            full = jnp.dot(grads[...], tile, preferred_element_type=jnp.float32)
            rows = full.shape[0] // 2
            for k in range(4):
                block = (full[:, k * BLOCK : (k + 1) * BLOCK] * gain[:, columns[k]]).astype(jnp.bfloat16)
                there = self.second(colour, k)
                send[len(self.distances) - 1 - at, colour, lax.rem(4 - there, 4), low] = block[:rows]
                own[at, colour, there, low] = block[rows:]
            return carry

        lax.fori_loop(0, self.count, body, 0)


def first_kernel(factor, place, tokens, keys, gain, send, own, held, grads, scaled, load):
    count, width = tokens.shape

    def rows_of(i):
        return pl.ds(pl.multiple_of(i * ROWS_AT_A_TIME, ROWS_AT_A_TIME), ROWS_AT_A_TIME)

    def read(i):
        return pltpu.make_async_copy(tokens.at[rows_of(i)], held.at[rows_of(i)], load.at[i])

    for i in range(count // ROWS_AT_A_TIME):
        read(i).start()

    def squares(i, carry):
        read(i).wait()
        rows = rows_of(i)

        def add(j, total):
            for k in range(8):
                part = held[rows, pl.ds(pl.multiple_of((j * 8 + k) * BLOCK, BLOCK), BLOCK)].astype(jnp.float32)
                total = total + part * part
            return total

        total = jnp.zeros((ROWS_AT_A_TIME, BLOCK), jnp.float32)
        total = lax.fori_loop(0, width // (8 * BLOCK), add, total)
        meansq = jnp.sum(total, axis=1, keepdims=True) / width
        scale = lax.rsqrt(meansq + norm_epsilon) * factor
        scaled[rows] = keys[rows].astype(jnp.float32) * scale
        return carry

    lax.fori_loop(0, count // ROWS_AT_A_TIME, squares, 0)

    core = place[3]
    for group in range(4):
        mine = jnp.where(core == group % 2, 2, 0)
        at = pl.ds(pl.multiple_of((mine + group // 2) * BLOCK, BLOCK), BLOCK)
        for t in range(count // BLOCK):
            square = scaled[t * BLOCK : (t + 1) * BLOCK, group * BLOCK : (group + 1) * BLOCK]
            grads[at, t * BLOCK : (t + 1) * BLOCK] = square.T.astype(jnp.bfloat16)

    Tiles(place, (2,)).products(held, grads, gain, send, own)


def later_kernel(distances, place, tokens, grads, gain, send, own):
    Tiles(place, distances).products(tokens, grads, gain, send, own)


def terms(kernel, distances, outs, scratch, tokens_in, limit, place, tokens, grads, gain):
    count = tokens.shape[0]
    cols = 4 * BLOCK
    part = jax.ShapeDtypeStruct((len(distances), 2, 4, 2, cols // 2, BLOCK), jnp.bfloat16)
    in_vmem = pl.BlockSpec(memory_space=pltpu.VMEM)
    in_smem = pl.BlockSpec(memory_space=pltpu.SMEM)
    outs = [part, part] + outs
    flops = 2 * len(distances) * 16 * BLOCK * count * cols
    return pl.pallas_call(
        kernel,
        out_shape=outs,
        in_specs=[in_smem, pl.BlockSpec(memory_space=tokens_in), in_vmem, in_vmem],
        out_specs=[in_vmem] * len(outs),
        scratch_shapes=scratch,
        cost_estimate=pl.CostEstimate(flops=flops, bytes_accessed=2**20, transcendentals=0),
        compiler_params=pltpu.CompilerParams(vmem_limit_bytes=limit * 2**20),
    )(place, tokens, grads, gain)


def first_terms(place, tokens, keys, gain, factor):
    count, cols = keys.shape
    outs = [jax.ShapeDtypeStruct(tokens.shape, jnp.bfloat16), jax.ShapeDtypeStruct((cols, count), jnp.bfloat16)]
    scratch = [pltpu.VMEM((count, cols), jnp.float32), pltpu.SemaphoreType.DMA((count // ROWS_AT_A_TIME,))]
    kernel = functools.partial(first_kernel, factor)
    return terms(kernel, (2,), outs, scratch, pl.ANY, FIRST_LIMIT, place, tokens, keys, gain)


def later_terms(distances, place, tokens, grads, gain):
    kernel = functools.partial(later_kernel, distances)
    return terms(kernel, distances, [], [], pltpu.VMEM, LATER_LIMIT, place, tokens, grads, gain)


def ring_sum(terms, axis):
    others = [onward(terms[s], axis, s) for s in (2, 1, 3)]
    return wide(terms[0]) + sum(wide(other) for other in others)


def per_device(tokens, keys_grad, norm_gain, weight, momentum):
    x, zl, y, zh, core = (lax.axis_index(a) for a in FSDP + GROUP)
    rows, cols = momentum.shape
    groups = lax.axis_size(GROUP)
    factor = inner_rate / math.sqrt(lax.axis_size(FSDP) * tokens.shape[1]) / groups
    place = jnp.stack([x, zl, y, core]).astype(jnp.int32)
    gain = norm_gain[None, :]
    axes = ("x", "y")

    send, own, held, grads = first_terms(place, tokens[0], keys_grad[0], gain, factor)
    received = swap(send, "core")
    far = [None, None]
    for c in (0, 1):
        far[c] = onward(narrow(wide(own[0, c]) + wide(received[0, c])), axes[c], 1)

    send, own = later_terms((1, 3), place, held, grads, gain)
    received = swap(send, "core")
    sides = [[wide(own[i, c]) + wide(received[i, c]) for i in (0, 1)] for c in (0, 1)]
    back = [None, None]
    for c in (0, 1):
        back[c] = onward(narrow(sides[c][1]), axes[c], -1)

    front = [None, None]
    for c in (0, 1):
        front[c] = onward(narrow(sides[c][0] + wide(far[c])), axes[c], 1)

    send, own = later_terms((0,), place, held, grads, gain)
    received = swap(send, "core")
    sums = [narrow(wide(own[0, c]) + wide(received[0, c]) + wide(back[c]) + wide(front[c])) for c in (0, 1)]

    sums = [ring_sum(sums[0], "y"), ring_sum(sums[1], "x")]
    lines = [sums[0][0], sums[0][1], sums[1][0], sums[1][1]]
    partial = lines[0]
    for step in (1, 2, 3):
        partial += wide(shift(narrow(lines[step]), "zl", step))

    partial = partial.reshape(2, cols, rows)
    both_rate = 1 + momentum_decay
    mine = (jnp.arange(2) == zh)[:, None, None]
    joined = narrow(partial + jnp.where(mine, momentum.T * (momentum_decay**2 / both_rate), 0.0))
    received = swap(joined, "zh")
    update = wide(joined) + wide(received)
    updates = jnp.stack([update, swap(update, "core")])
    updates = jnp.where(core == 0, updates, updates[::-1])
    average = jnp.where(zh == 0, partial[0] + wide(received[0]), partial[1] + wide(received[1]))

    new_momentum = momentum_decay * momentum + average.T
    updates = updates.transpose(3, 1, 0, 2).reshape(rows, 4 * cols)
    new_weight = narrow(wide(weight) - outer_rate * both_rate * updates)
    return (new_weight, new_momentum)


def solution(mesh):
    finer = Mesh(mesh.devices.reshape(2, 2, 4, 4, 4), GROUP + FSDP)
    in_specs = (
        P(GROUP, FSDP, None),
        P(GROUP, FSDP, None),
        P(),
        P(FSDP, None),
        P(FSDP, GROUP),
    )
    out_specs = (P(FSDP, None), P(FSDP, GROUP))
    return jax.shard_map(per_device, mesh=finer, in_specs=in_specs, out_specs=out_specs, check_vma=False)
```

```python
import functools
import math

import jax
import jax.numpy as jnp
from jax import lax
from jax.experimental import pallas as pl
from jax.experimental.pallas import tpu as pltpu
from jax.sharding import Mesh
from jax.sharding import PartitionSpec as P


BLOCK = 128
ROWS_AT_A_TIME = 64
FIRST_LIMIT = 38
LATER_LIMIT = 24
FSDP = ("x", "zl", "y")
GROUP = ("zh", "core")

norm_epsilon = 1e-05
inner_rate = 0.5
outer_rate = 0.7
momentum_decay = 0.9


def shift(block, axis, step):
    count = lax.axis_size(axis)
    return lax.ppermute(block, axis, [(i, (i + step) % count) for i in range(count)])


def onward(block, axis, step):
    route = [(i, (i + step) % 4) for i in range(4)] + [(4 + i, 4 + (i - step) % 4) for i in range(4)]
    return lax.ppermute(block, ("core", axis), route)


def swap(block, axis):
    return lax.ppermute(block, axis, [(0, 1), (1, 0)])


def wide(array):
    return array.astype(jnp.float32)


def narrow(array):
    return array.astype(jnp.bfloat16)


class Tiles:
    def __init__(self, place, distances, colours=(0, 1)):
        self.x, self.zl, self.y, self.core = (place[i] for i in range(4))
        self.distances, self.colours = distances, colours
        self.count = 2 * len(colours) * len(distances)

    def parts(self, turn):
        count = len(self.colours)
        return turn // (2 * count), (turn // 2) % count, turn % 2

    def column(self, turn, block):
        at, colour, low = self.parts(turn)
        colour = colour + self.colours[0]
        distance = self.distances[0] + 2 * at
        along = jnp.where(colour == 0, self.x, self.y)
        along = lax.rem(along + 4 + jnp.where(self.core == 0, distance, -distance), 4)
        line = lax.rem(self.zl + 2 * colour + low, 4)
        x, y = jnp.where(colour == 0, along, block), jnp.where(colour == 0, block, along)
        return pl.multiple_of(((x * 4 + line) * 4 + y) * BLOCK, BLOCK)

    def second(self, colour, block):
        across = jnp.where(colour == 0, self.y, self.x)
        return lax.rem(jnp.where(self.core == 0, block - across, across - block) + 4, 4)

    def products(self, tokens, grads, gain, send, own):
        def body(turn, carry):
            at, colour, low = self.parts(turn)
            columns = [pl.ds(self.column(turn, k), BLOCK) for k in range(4)]
            tile = jnp.concatenate([tokens[:, c] for c in columns], axis=1)
            full = jnp.dot(grads[...], tile, preferred_element_type=jnp.float32)
            rows = full.shape[0] // 2
            for k in range(4):
                block = (full[:, k * BLOCK : (k + 1) * BLOCK] * gain[:, columns[k]]).astype(jnp.bfloat16)
                there = self.second(colour + self.colours[0], k)
                send[len(self.distances) - 1 - at, colour, lax.rem(4 - there, 4), low] = block[:rows]
                own[at, colour, there, low] = block[rows:]
            return carry

        lax.fori_loop(0, self.count, body, 0)


def first_kernel(factor, place, tokens, keys, gain, send, own, held, grads, scaled, load):
    count, width = tokens.shape

    def rows_of(i):
        return pl.ds(pl.multiple_of(i * ROWS_AT_A_TIME, ROWS_AT_A_TIME), ROWS_AT_A_TIME)

    def read(i):
        return pltpu.make_async_copy(tokens.at[rows_of(i)], held.at[rows_of(i)], load.at[i])

    for i in range(count // ROWS_AT_A_TIME):
        read(i).start()

    def squares(i, carry):
        read(i).wait()
        rows = rows_of(i)

        def add(j, total):
            for k in range(8):
                part = held[rows, pl.ds(pl.multiple_of((j * 8 + k) * BLOCK, BLOCK), BLOCK)].astype(jnp.float32)
                total = total + part * part
            return total

        total = jnp.zeros((ROWS_AT_A_TIME, BLOCK), jnp.float32)
        total = lax.fori_loop(0, width // (8 * BLOCK), add, total)
        meansq = jnp.sum(total, axis=1, keepdims=True) / width
        scale = lax.rsqrt(meansq + norm_epsilon) * factor
        scaled[rows] = keys[rows].astype(jnp.float32) * scale
        return carry

    lax.fori_loop(0, count // ROWS_AT_A_TIME, squares, 0)

    core = place[3]
    for group in range(4):
        mine = jnp.where(core == group % 2, 2, 0)
        at = pl.ds(pl.multiple_of((mine + group // 2) * BLOCK, BLOCK), BLOCK)
        for t in range(count // BLOCK):
            square = scaled[t * BLOCK : (t + 1) * BLOCK, group * BLOCK : (group + 1) * BLOCK]
            grads[at, t * BLOCK : (t + 1) * BLOCK] = square.T.astype(jnp.bfloat16)

    Tiles(place, (2,)).products(held, grads, gain, send, own)


def later_kernel(distances, colours, place, tokens, grads, gain, send, own):
    Tiles(place, distances, colours).products(tokens, grads, gain, send, own)


def terms(kernel, distances, colours, outs, scratch, tokens_in, limit, place, tokens, grads, gain):
    count = tokens.shape[0]
    cols = 4 * BLOCK
    part = jax.ShapeDtypeStruct((len(distances), len(colours), 4, 2, cols // 2, BLOCK), jnp.bfloat16)
    in_vmem = pl.BlockSpec(memory_space=pltpu.VMEM)
    in_smem = pl.BlockSpec(memory_space=pltpu.SMEM)
    outs = [part, part] + outs
    flops = 2 * len(distances) * len(colours) * 8 * BLOCK * count * cols
    return pl.pallas_call(
        kernel,
        out_shape=outs,
        in_specs=[in_smem, pl.BlockSpec(memory_space=tokens_in), in_vmem, in_vmem],
        out_specs=[in_vmem] * len(outs),
        scratch_shapes=scratch,
        cost_estimate=pl.CostEstimate(flops=flops, bytes_accessed=2**20, transcendentals=0),
        compiler_params=pltpu.CompilerParams(vmem_limit_bytes=limit * 2**20),
    )(place, tokens, grads, gain)


def first_terms(place, tokens, keys, gain, factor):
    count, cols = keys.shape
    outs = [jax.ShapeDtypeStruct(tokens.shape, jnp.bfloat16), jax.ShapeDtypeStruct((cols, count), jnp.bfloat16)]
    scratch = [pltpu.VMEM((count, cols), jnp.float32), pltpu.SemaphoreType.DMA((count // ROWS_AT_A_TIME,))]
    kernel = functools.partial(first_kernel, factor)
    return terms(kernel, (2,), (0, 1), outs, scratch, pl.ANY, FIRST_LIMIT, place, tokens, keys, gain)


def later_terms(distances, colours, place, tokens, grads, gain):
    kernel = functools.partial(later_kernel, distances, colours)
    return terms(kernel, distances, colours, [], [], pltpu.VMEM, LATER_LIMIT, place, tokens, grads, gain)


def ring_sum(terms, axis):
    others = [onward(terms[s], axis, s) for s in (2, 1, 3)]
    return wide(terms[0]) + sum(wide(other) for other in others)


def per_device(tokens, keys_grad, norm_gain, weight, momentum):
    x, zl, y, zh, core = (lax.axis_index(a) for a in FSDP + GROUP)
    rows, cols = momentum.shape
    groups = lax.axis_size(GROUP)
    factor = inner_rate / math.sqrt(lax.axis_size(FSDP) * tokens.shape[1]) / groups
    place = jnp.stack([x, zl, y, core]).astype(jnp.int32)
    gain = norm_gain[None, :]
    axes = ("x", "y")

    send, own, held, grads = first_terms(place, tokens[0], keys_grad[0], gain, factor)
    received = swap(send, "core")
    far = [None, None]
    for c in (0, 1):
        far[c] = onward(narrow(wide(own[0, c]) + wide(received[0, c])), axes[c], 1)

    sides, back = [None, None], [None, None]
    for c in (0, 1):
        send, own = later_terms((1, 3), (c,), place, held, grads, gain)
        received = swap(send, "core")
        sides[c] = [wide(own[i, 0]) + wide(received[i, 0]) for i in (0, 1)]
        back[c] = onward(narrow(sides[c][1]), axes[c], -1)

    front = [None, None]
    for c in (0, 1):
        front[c] = onward(narrow(sides[c][0] + wide(far[c])), axes[c], 1)

    send, own = later_terms((0,), (0, 1), place, held, grads, gain)
    received = swap(send, "core")
    sums = [narrow(wide(own[0, c]) + wide(received[0, c]) + wide(back[c]) + wide(front[c])) for c in (0, 1)]

    sums = [ring_sum(sums[0], "y"), ring_sum(sums[1], "x")]
    lines = [sums[0][0], sums[0][1], sums[1][0], sums[1][1]]
    partial = lines[0]
    for step in (1, 2, 3):
        partial += wide(shift(narrow(lines[step]), "zl", step))

    partial = partial.reshape(2, cols, rows)
    both_rate = 1 + momentum_decay
    mine = (jnp.arange(2) == zh)[:, None, None]
    joined = narrow(partial + jnp.where(mine, momentum.T * (momentum_decay**2 / both_rate), 0.0))
    received = swap(joined, "zh")
    update = wide(joined) + wide(received)
    updates = jnp.stack([update, swap(update, "core")])
    updates = jnp.where(core == 0, updates, updates[::-1])
    average = jnp.where(zh == 0, partial[0] + wide(received[0]), partial[1] + wide(received[1]))

    new_momentum = momentum_decay * momentum + average.T
    updates = updates.transpose(3, 1, 0, 2).reshape(rows, 4 * cols)
    new_weight = narrow(wide(weight) - outer_rate * both_rate * updates)
    return (new_weight, new_momentum)


def solution(mesh):
    finer = Mesh(mesh.devices.reshape(2, 2, 4, 4, 4), GROUP + FSDP)
    in_specs = (
        P(GROUP, FSDP, None),
        P(GROUP, FSDP, None),
        P(),
        P(FSDP, None),
        P(FSDP, GROUP),
    )
    out_specs = (P(FSDP, None), P(FSDP, GROUP))
    return jax.shard_map(per_device, mesh=finer, in_specs=in_specs, out_specs=out_specs, check_vma=False)
```
